8 devices in a mesh: dp: 1 (over z), cy: 2 (over y), cx: 4 (over x, core).
Axes of the slice: x: 2, y: 2, z: 1, core: 2. Of those that a mesh axis runs over, the one named last changes fastest.
Arguments:
- queries: bfloat16 [16384, 12, 128], P(('dp', 'cx', 'cy'))
- keys: bfloat16 [16384, 2, 128], P(('dp', 'cx', 'cy'))
- values: bfloat16 [16384, 2, 128], P(('dp', 'cx', 'cy'))
- doc_ids: int32 [16384], P(('dp', 'cx', 'cy'))
Outputs:
- output: bfloat16 [16384, 12, 128], P(('dp', 'cx', 'cy'))
All inputs are finite; a program needn't handle non-finite values.
Results may differ from the reference program's by a relative error of at most 0.00125057.
Values are sent between devices in bfloat16 or wider.
A program may use at most 1 GiB of HBM per device.

```python
import jax
import jax.numpy as jnp
from jax import lax

SEQ_LEN = 16384
GROUP_SIZE = 8
HEADS = 12
KV_HEADS = 2
HEAD_DIM = 128
DOC_COUNT = 6
ROW_BLOCK = 16

TOKENS_DEV = SEQ_LEN // GROUP_SIZE
PIECE_LEN = TOKENS_DEV // 2
Q_PER_KV = HEADS // KV_HEADS


def layout_positions():
    row_ids = jnp.arange(SEQ_LEN)
    dev_rank = row_ids // TOKENS_DEV
    in_dev = row_ids % TOKENS_DEV
    piece_ids = jnp.where(in_dev < PIECE_LEN, dev_rank, 2 * GROUP_SIZE - 1 - dev_rank)
    return piece_ids * PIECE_LEN + in_dev % PIECE_LEN


def draw_segments(seg_key):
    cut_points = jax.random.permutation(seg_key, SEQ_LEN - 1)[:DOC_COUNT - 1] + 1
    return jnp.sum(layout_positions()[:, None] >= cut_points[None, :], axis=1).astype(jnp.int32)


def setup_inputs(seed: int = 0, part: int = 0) -> dict:
    part_key = jax.random.fold_in(jax.random.key(seed), part)
    key_q, key_k, key_v, key_shift, key_seg = jax.random.split(part_key, 5)
    q_arr = jax.random.normal(key_q, (SEQ_LEN, HEADS, HEAD_DIM), jnp.float32)
    k_arr = jax.random.normal(key_k, (SEQ_LEN, KV_HEADS, HEAD_DIM), jnp.float32)
    v_noise = jax.random.normal(key_v, (2 * GROUP_SIZE, PIECE_LEN, KV_HEADS, HEAD_DIM), jnp.float32)
    v_shift = jax.random.normal(key_shift, (2 * GROUP_SIZE, 1, KV_HEADS, HEAD_DIM), jnp.float32)
    v_arr = (v_noise + v_shift).reshape(SEQ_LEN, KV_HEADS, HEAD_DIM)
    return {'queries': q_arr.astype(jnp.bfloat16), 'keys': k_arr.astype(jnp.bfloat16), 'values': v_arr.astype(jnp.bfloat16), 'doc_ids': draw_segments(key_seg)}


def reference(queries, keys, values, doc_ids):
    positions = layout_positions()
    score_scale = HEAD_DIM ** -0.5
    keys_f32 = keys.astype(jnp.float32)
    vals_f32 = values.astype(jnp.float32)
    q_blocks = queries.reshape(SEQ_LEN // ROW_BLOCK, ROW_BLOCK, KV_HEADS, Q_PER_KV, HEAD_DIM)
    pos_blocks = positions.reshape(SEQ_LEN // ROW_BLOCK, ROW_BLOCK)
    doc_blocks = doc_ids.reshape(SEQ_LEN // ROW_BLOCK, ROW_BLOCK)

    def one_block(block_in):
        q_blk, q_pos, q_doc = block_in
        scores = jnp.einsum('qgjd,kgd->qgjk', q_blk.astype(jnp.float32), keys_f32) * score_scale
        allowed = (positions[None, :] <= q_pos[:, None]) & (doc_ids[None, :] == q_doc[:, None])
        key_mask = allowed[:, None, None, :]
        row_max = jnp.max(jnp.where(key_mask, scores, -1e30), axis=-1, keepdims=True)
        weights = jnp.exp(jnp.where(key_mask, scores - row_max, -1e30))
        denominator = jnp.sum(weights, axis=-1)
        numerator = jnp.einsum('qgjk,kgd->qgjd', weights.astype(jnp.bfloat16).astype(jnp.float32), vals_f32)
        return (numerator / denominator[..., None]).astype(jnp.bfloat16)

    out_blocks = lax.map(one_block, (q_blocks, pos_blocks, doc_blocks))
    return out_blocks.reshape(SEQ_LEN, HEADS, HEAD_DIM)
```

```python
import functools

import jax
import jax.numpy as jnp
from jax import lax
from jax.experimental import pallas as pl
from jax.experimental.pallas import tpu as pltpu
from jax.sharding import PartitionSpec as P

NEG_BIG = -1e30
LOG2E = 1.4426950408889634
DOCS = 6
TILE = 256
BLOCK = 512
CHUNK = 256
MAX_ITEMS = 256


def fold8(x, op):
    return op(x.reshape(x.shape[0] // 8, 8, x.shape[1]), axis=0)


def attend_kernel(
    masks, group, first_stage, last_stage,
    rank_ref, cnt_ref, qd_ref, qdoc_ref, q_hbm, k_hbm, v_hbm, *rest,
):
    n_in = 0 if first_stage else 3
    n_out = 1 if last_stage else 3
    state_in, rest = rest[:n_in], rest[n_in:]
    outs, rest = rest[:n_out], rest[n_out:]
    q_ref, k_ref, v_ref, s_ref, mx_ref, m_ref, l_ref, acc_ref, o_ref, it_tile, it_sp, it_start, it_mask, sems = rest
    n_src = len(masks)
    n_tiles, n_pairs = q_ref.shape[0], q_ref.shape[1]
    per_kv = n_pairs // 2
    piece = k_ref.shape[2] // 2
    tiles_per_piece = piece // TILE
    scale = q_ref.shape[-1] ** -0.5 * LOG2E
    rank = rank_ref[0]

    copies = [pltpu.make_async_copy(q_hbm, q_ref, sems.at[0])]
    copies += [pltpu.make_async_copy(k_hbm, k_ref, sems.at[1]), pltpu.make_async_copy(v_hbm, v_ref, sems.at[2])]
    if not first_stage:
        copies += [pltpu.make_async_copy(a, b, sems.at[3 + i]) for i, (a, b) in enumerate(zip(state_in, (m_ref, l_ref, acc_ref)))]
    for copy in copies:
        copy.start()

    def list_tile(tile, count):
        half = tile // tiles_per_piece
        off = (tile % tiles_per_piece) * TILE
        q_piece = jnp.where(half == 0, rank, 2 * group - 1 - rank)
        d_first, d_last = qd_ref[2 * tile], qd_ref[2 * tile + 1]
        for src in range(n_src):
            src_rank = rank ^ masks[src]
            for k_half in range(2):
                sp = 2 * src + k_half
                k_piece = src_rank if k_half == 0 else 2 * group - 1 - src_rank
                lo = cnt_ref[sp * DOCS + d_first]
                lo_last = cnt_ref[sp * DOCS + d_last]
                diag = k_piece == q_piece
                hi = jnp.where(diag, off + TILE, piece)
                need = jnp.where(jnp.logical_and(k_piece <= q_piece, lo < hi), hi - (lo // 128) * 128, 0)
                blocks = (need + BLOCK - 1) // BLOCK
                start0 = jnp.maximum(hi - BLOCK * blocks, 0)

                def add(i, at, sp=sp, start0=start0, diag=diag, lo_last=lo_last):
                    start = start0 + i * BLOCK
                    it_tile[at] = tile
                    it_sp[at] = sp
                    it_start[at] = start
                    cut = jnp.logical_or(start < lo_last, jnp.logical_and(diag, start + BLOCK > off + 1))
                    it_mask[at] = jnp.where(cut, jnp.where(diag, 2, 1), 0)
                    return at + 1

                count = lax.fori_loop(0, blocks, add, count)
        return count

    count = lax.fori_loop(0, n_tiles, list_tile, 0)

    if first_stage:
        m_ref[...] = jnp.full_like(m_ref, NEG_BIG)
        l_ref[...] = jnp.zeros_like(l_ref)
        acc_ref[...] = jnp.zeros_like(acc_ref)
    for copy in copies:
        copy.wait()

    def score_chunk(tile, sp, start, h, j):
        src, base = sp // 2, (sp % 2) * piece
        rows = pl.ds(pl.multiple_of(base + start + j * CHUNK, 128), CHUNK)
        return lax.dot_general(
            k_ref[src, h // per_kv, rows, :], q_ref[tile, h], (((1,), (1,)), ((), ())), preferred_element_type=jnp.float32
        )

    def values_chunk(sp, start, h, j):
        src, base = sp // 2, (sp % 2) * piece
        return v_ref[src, h // per_kv, :, pl.ds(pl.multiple_of(base + start + j * CHUNK, 128), CHUNK)]

    n_chunks = BLOCK // CHUNK

    @pl.when(count > 0)
    def prologue():
        for h in range(n_pairs):
            top = None
            for j in range(n_chunks):
                s = score_chunk(it_tile[0], it_sp[0], it_start[0], h, j)
                s_ref[h, j * CHUNK:(j + 1) * CHUNK, :] = s
                part = fold8(s, jnp.max)
                top = part if top is None else jnp.maximum(top, part)
            mx_ref[h] = top

    def body(t, masked):
        tile, sp, start = it_tile[t], it_sp[t], it_start[t]
        nxt = jnp.minimum(t + 1, count - 1)
        n_tile, n_sp, n_start = it_tile[nxt], it_sp[nxt], it_start[nxt]
        if masked:
            q_doc = qdoc_ref[tile]
            low = jnp.zeros_like(q_doc)
            for d in range(DOCS):
                low = jnp.where(q_doc == d, cnt_ref[sp * DOCS + d], low)
            off = (tile % tiles_per_piece) * TILE
            token = lax.broadcasted_iota(jnp.int32, q_doc.shape, 1) % TILE + off
            high = jnp.where(it_mask[t] == 2, token, piece)

            def allowed(j):
                k_idx = lax.broadcasted_iota(jnp.int32, (CHUNK, q_doc.shape[1]), 0) + (start + j * CHUNK)
                return jnp.logical_and(k_idx >= low, k_idx <= high)

        for h in range(n_pairs):
            if masked:
                top = None
                for j in range(n_chunks):
                    part = fold8(jnp.where(allowed(j), s_ref[h, j * CHUNK:(j + 1) * CHUNK, :], NEG_BIG), jnp.max)
                    top = part if top is None else jnp.maximum(top, part)
            else:
                top = mx_ref[h]
            m_old = m_ref[tile, h]
            m_new = jnp.maximum(m_old, jnp.max(top, axis=0, keepdims=True) * scale)
            rescale = jnp.exp2(m_old - m_new)
            m_ref[tile, h] = m_new
            total = l_ref[tile, h] * rescale
            part_acc = None
            new_top = None
            for j in range(n_chunks):
                p = jnp.exp2(s_ref[h, j * CHUNK:(j + 1) * CHUNK, :] * scale - m_new)
                if masked:
                    p = jnp.where(allowed(j), p, 0.0)
                total = total + fold8(p, jnp.sum)
                prod = jnp.dot(values_chunk(sp, start, h, j), p.astype(jnp.bfloat16), preferred_element_type=jnp.float32)
                part_acc = prod if part_acc is None else part_acc + prod
                s = score_chunk(n_tile, n_sp, n_start, h, j)
                s_ref[h, j * CHUNK:(j + 1) * CHUNK, :] = s
                part = fold8(s, jnp.max)
                new_top = part if new_top is None else jnp.maximum(new_top, part)
            mx_ref[h] = new_top
            l_ref[tile, h] = total
            acc_ref[tile, h] = acc_ref[tile, h] * rescale + part_acc

    def step(t, carry):
        masked = it_mask[t] > 0
        pl.when(masked)(lambda: body(t, True))
        pl.when(jnp.logical_not(masked))(lambda: body(t, False))
        return carry

    lax.fori_loop(0, count, step, 0)

    if last_stage:
        def finish(tile, carry):
            for h in range(n_pairs):
                denom = jnp.sum(l_ref[tile, h], axis=0, keepdims=True)
                o_ref[tile, h] = (acc_ref[tile, h] / denom).T.astype(o_ref.dtype)
            return carry

        lax.fori_loop(0, n_tiles, finish, 0)
        ends = [pltpu.make_async_copy(o_ref, outs[0], sems.at[0])]
    else:
        ends = [pltpu.make_async_copy(a, b, sems.at[i]) for i, (a, b) in enumerate(zip((m_ref, l_ref, acc_ref), outs))]
    for copy in ends:
        copy.start()
    for copy in ends:
        copy.wait()


def attend(masks, group, rank, cnt, qd, qdoc, q, k, v, state, last):
    n_tiles, n_pairs, cols, dim = q.shape
    stat = [(n_tiles, n_pairs, 1, cols), (n_tiles, n_pairs, 8, cols), (n_tiles, n_pairs, dim, cols)]
    if last:
        out_shape = [jax.ShapeDtypeStruct(q.shape, jnp.bfloat16)]
    else:
        out_shape = [jax.ShapeDtypeStruct(shape, jnp.float32) for shape in stat]
    state = () if state is None else tuple(state)
    any_spec = pl.BlockSpec(memory_space=pl.ANY)
    smem = pl.BlockSpec(memory_space=pltpu.SMEM)
    vmem = pl.BlockSpec(memory_space=pltpu.VMEM)
    items = 2 * n_tiles * 2 * len(masks)
    flops = len(masks) * 2 * 10**9
    return pl.pallas_call(
        functools.partial(attend_kernel, masks, group, not state, last),
        out_shape=out_shape,
        in_specs=[smem, smem, smem, vmem, any_spec, any_spec, any_spec] + [any_spec] * len(state),
        out_specs=[any_spec] * len(out_shape),
        scratch_shapes=[
            pltpu.VMEM(q.shape, q.dtype),
            pltpu.VMEM(k.shape, k.dtype),
            pltpu.VMEM(v.shape, v.dtype),
            pltpu.VMEM((n_pairs, BLOCK, cols), jnp.float32),
            pltpu.VMEM((n_pairs, 8, cols), jnp.float32),
            *[pltpu.VMEM(shape, jnp.float32) for shape in stat],
            pltpu.VMEM(q.shape if last else (8, 128), jnp.bfloat16),
            *[pltpu.SMEM((items,), jnp.int32)] * 4,
            pltpu.SemaphoreType.DMA((6,)),
        ],
        compiler_params=pltpu.CompilerParams(vmem_limit_bytes=60 * 1024 * 1024),
        cost_estimate=pl.CostEstimate(flops=flops, bytes_accessed=20 << 20, transcendentals=0),
    )(rank, cnt, qd, qdoc, q, k, v, *state)


def solution(mesh):
    size_cx, size_cy = mesh.shape['cx'], mesh.shape['cy']
    group = size_cx * size_cy
    seq_spec = P(('dp', 'cx', 'cy'), None, None)

    def per_device(q_loc, k_loc, v_loc, doc_loc):
        tok, heads, dim = q_loc.shape
        kv_heads = k_loc.shape[1]
        piece = tok // 2
        n_tiles = tok // TILE
        rank = lax.axis_index('cx') * size_cy + lax.axis_index('cy')
        q = q_loc.reshape(n_tiles, TILE, heads // 2, 2, dim).transpose(0, 2, 3, 1, 4).reshape(n_tiles, heads // 2, 2 * TILE, dim)
        k = k_loc.transpose(1, 0, 2)
        v = v_loc.transpose(1, 2, 0)
        doc_tiles = doc_loc.reshape(n_tiles, 1, TILE)
        qdoc = jnp.concatenate([doc_tiles, doc_tiles], axis=2)
        qd = jnp.stack([doc_tiles[:, 0, 0], doc_tiles[:, 0, -1]], axis=1).reshape(-1)
        cnt = jnp.sum(doc_loc.reshape(2, 1, piece) < jnp.arange(DOCS)[None, :, None], axis=-1).astype(jnp.int32)
        gather = functools.partial(lax.all_gather, axis_name=('cx', 'cy'))
        k_all, v_all, cnt_all = gather(k), gather(v), gather(cnt)
        order = jnp.arange(group) ^ rank
        cnt_all = cnt_all[order]
        k_all, v_all = k_all[order], v_all[order]
        out, = attend(tuple(range(group)), group, rank[None], cnt_all.reshape(-1), qd, qdoc, q, k_all, v_all, None, True)
        out = out.reshape(n_tiles, heads // 2, 2, TILE, dim).transpose(0, 3, 1, 2, 4)
        return out.reshape(tok, heads, dim)

    return jax.shard_map(per_device, mesh=mesh, in_specs=(seq_spec, seq_spec, seq_spec, P(('dp', 'cx', 'cy'))), out_specs=seq_spec, check_vma=False)
```

```python
import functools

import jax
import jax.numpy as jnp
from jax import lax
from jax.experimental import pallas as pl
from jax.experimental.pallas import tpu as pltpu
from jax.sharding import PartitionSpec as P

FLOOR = -1e30
MASKED = -3e38
LOG2E = 1.4426950408889634
DOCS = 6
TILE = 512
BLOCK = 512
CHUNK = 256


def fold8(x, op):
    return op(x.reshape(x.shape[0] // 8, 8, x.shape[1]), axis=0)


def attend_kernel(masks, group, first, last, rank_ref, cq_ref, cnt_ref, *rest):
    n_src = len(masks)
    q_hbm, rest = rest[:2], rest[2:]
    kv_hbm, rest = rest[:n_src], rest[n_src:]
    if not first:
        state_in, rest = rest[:2], rest[2:]
    outs, rest = rest[:2], rest[2:]
    q_ref, k_ref, v_ref, s_ref, mx_ref, ml_ref, acc_ref, o_ref, it_tile, it_sp, it_start, it_mask, it_from, sems, in_sems, out_sems = rest
    n_tiles, heads = q_ref.shape[0], q_ref.shape[1]
    piece = k_ref.shape[1] // 2
    tiles_per_piece = piece // TILE
    scale = q_ref.shape[-1] ** -0.5 * LOG2E
    rank = rank_ref[0]
    half_tiles = n_tiles // 2

    loads = [
        pltpu.make_async_copy(q_hbm[0], q_ref.at[pl.ds(0, half_tiles)], sems.at[0]),
        pltpu.make_async_copy(q_hbm[1], q_ref.at[pl.ds(half_tiles, half_tiles)], sems.at[1]),
    ]
    for src in range(n_src):
        loads.append(pltpu.make_async_copy(kv_hbm[src].at[pl.ds(0, 2 * piece)], k_ref.at[src], sems.at[2 + 2 * src]))
        loads.append(pltpu.make_async_copy(kv_hbm[src].at[pl.ds(2 * piece, 2 * piece)], v_ref.at[src], sems.at[3 + 2 * src]))
    for copy in loads:
        copy.start()

    def doc_of(tile, token):
        first_of = (tile // tiles_per_piece) * DOCS
        return sum((token >= cq_ref[first_of + d]).astype(jnp.int32) for d in range(1, DOCS))

    def list_tile(tile, count):
        it_from[tile] = count
        q_rank = jnp.where(tile < half_tiles, rank, rank ^ 2)
        q_piece = jnp.where((tile // tiles_per_piece) % 2 == 0, q_rank, 2 * group - 1 - q_rank)
        off = (tile % tiles_per_piece) * TILE
        d_first, d_last = doc_of(tile, off), doc_of(tile, off + TILE - 1)
        for sp in range(2 * n_src):
            src_rank = rank ^ masks[sp // 2]
            k_piece = src_rank if sp % 2 == 0 else 2 * group - 1 - src_rank
            lo, lo_last = cnt_ref[sp * DOCS + d_first], cnt_ref[sp * DOCS + d_last]
            diag = k_piece == q_piece
            hi = jnp.where(diag, off + TILE, piece)
            need = jnp.where(jnp.logical_and(k_piece <= q_piece, lo < hi), hi - (lo // 128) * 128, 0)
            blocks = (need + BLOCK - 1) // BLOCK
            start0 = jnp.maximum(hi - BLOCK * blocks, 0)

            def add(i, at, sp=sp, start0=start0, diag=diag, lo_last=lo_last):
                start = start0 + i * BLOCK
                it_tile[at] = tile
                it_sp[at] = sp
                it_start[at] = start
                cut = jnp.logical_or(start < lo_last, jnp.logical_and(diag, start + BLOCK > off + 1))
                it_mask[at] = jnp.where(cut, jnp.where(diag, 2, 1), 0)
                return at + 1

            count = lax.fori_loop(0, blocks, add, count)
        return count

    count = lax.fori_loop(0, n_tiles, list_tile, 0)
    it_from[n_tiles] = count

    def state_copies(tile, sem, inward):
        pairs = ((0, ml_ref), (1, acc_ref))
        if inward:
            return [pltpu.make_async_copy(state_in[i].at[tile], ref.at[tile], sem.at[i, tile]) for i, ref in pairs]
        return [pltpu.make_async_copy(ref.at[tile], outs[i].at[tile], sem.at[i, tile]) for i, ref in pairs]

    def used(tile):
        return it_from[tile + 1] > it_from[tile]

    def each_tile(fn):
        def one(tile, carry):
            if last:
                fn(tile)
            else:
                pl.when(used(tile))(lambda: fn(tile))
            return carry

        lax.fori_loop(0, n_tiles, one, 0)

    if first:
        ml_ref[:, :, 0:8, :] = jnp.zeros(ml_ref.shape[:2] + (8, TILE), jnp.float32)
        ml_ref[:, :, 8:16, :] = jnp.full(ml_ref.shape[:2] + (8, TILE), FLOOR, jnp.float32)
        acc_ref[...] = jnp.zeros_like(acc_ref)
    else:
        def fetch(tile):
            for copy in state_copies(tile, in_sems, True):
                copy.start()

        each_tile(fetch)
    for copy in loads:
        copy.wait()

    n_chunks = BLOCK // CHUNK

    def column(sp, start, j):
        return pl.ds(pl.multiple_of((sp % 2) * piece + start + j * CHUNK, 128), CHUNK)

    def values(sp, start, j):
        base = (sp % 2) * piece + start + j * CHUNK
        parts = [v_ref[sp // 2, pl.ds(pl.multiple_of(base + i * 128, 128), 128), :] for i in range(CHUNK // 128)]
        return jnp.concatenate(parts, axis=1)

    def limits(t):
        tile, sp, start = it_tile[t], it_sp[t], it_start[t]
        token = lax.broadcasted_iota(jnp.int32, (1, TILE), 1) + (tile % tiles_per_piece) * TILE
        low = jnp.full_like(token, cnt_ref[sp * DOCS])
        for d in range(1, DOCS):
            low = jnp.where(token >= cq_ref[(tile // tiles_per_piece) * DOCS + d], cnt_ref[sp * DOCS + d], low)
        return low - start, jnp.where(it_mask[t] == 2, token, piece) - start

    def score(t, h, j, bounds):
        s = lax.dot_general(
            k_ref[it_sp[t] // 2, column(it_sp[t], it_start[t], j), :], q_ref[it_tile[t], h],
            (((1,), (1,)), ((), ())), preferred_element_type=jnp.float32,
        )
        if bounds is not None:
            row = lax.broadcasted_iota(jnp.int32, s.shape, 0) + j * CHUNK
            s = jnp.where(jnp.logical_and(row >= bounds[0], row <= bounds[1]), s, MASKED)
        s_ref[h, j * CHUNK:(j + 1) * CHUNK, :] = s
        return fold8(s, jnp.max)

    @pl.when(count > 0)
    def prologue():
        bounds = limits(0)
        for h in range(heads):
            mx_ref[h] = functools.reduce(jnp.maximum, [score(0, h, j, bounds) for j in range(n_chunks)])

    def body(t, nxt, masked):
        tile, sp, start = it_tile[t], it_sp[t], it_start[t]
        bounds = limits(nxt) if masked else None
        for h in range(heads):
            m_old = ml_ref[tile, h, 8:9, :]
            m_new = jnp.maximum(m_old, jnp.max(mx_ref[h], axis=0, keepdims=True) * scale)
            rescale = jnp.exp2(m_old - m_new)
            ml_ref[tile, h, 8:9, :] = m_new
            total = ml_ref[tile, h, 0:8, :] * rescale
            prods, tops = [], []
            for j in range(n_chunks):
                p = jnp.exp2(s_ref[h, j * CHUNK:(j + 1) * CHUNK, :] * scale - m_new)
                total = total + fold8(p, jnp.sum)
                prods.append(jnp.dot(values(sp, start, j), p.astype(jnp.bfloat16), preferred_element_type=jnp.float32))
                tops.append(score(nxt, h, j, bounds))
            mx_ref[h] = functools.reduce(jnp.maximum, tops)
            ml_ref[tile, h, 0:8, :] = total
            acc_ref[tile, h] = acc_ref[tile, h] * rescale + functools.reduce(jnp.add, prods)

    def step(t, carry):
        nxt = jnp.minimum(t + 1, count - 1)
        masked = it_mask[nxt] > 0
        pl.when(masked)(lambda: body(t, nxt, True))
        pl.when(jnp.logical_not(masked))(lambda: body(t, nxt, False))
        return carry

    def out_copy(tile, dst, base):
        return pltpu.make_async_copy(o_ref.at[tile], dst.at[tile - base], out_sems.at[0, tile])

    def send_out(tile, act):
        pl.when(tile < half_tiles)(lambda: act(out_copy(tile, outs[0], 0)))
        pl.when(tile >= half_tiles)(lambda: act(out_copy(tile, outs[1], half_tiles)))

    def run_tile(tile):
        if not first:
            for copy in state_copies(tile, in_sems, True):
                copy.wait()
        lax.fori_loop(it_from[tile], it_from[tile + 1], step, 0)
        if last:
            for h in range(heads):
                denom = jnp.sum(ml_ref[tile, h, 0:8, :], axis=0, keepdims=True)
                o_ref[tile, h] = (acc_ref[tile, h] / denom).T.astype(o_ref.dtype)
            send_out(tile, lambda copy: copy.start())
        else:
            for copy in state_copies(tile, out_sems, False):
                copy.start()

    each_tile(run_tile)

    def settle(tile):
        if last:
            send_out(tile, lambda copy: copy.wait())
        else:
            for copy in state_copies(tile, out_sems, False):
                copy.wait()

    each_tile(settle)


def attend(masks, group, rank, cq, cnt, q, kvs, state, last):
    half_tiles, heads, _, dim = q[1].shape
    n_tiles, n_src = 2 * half_tiles, len(masks)
    first = state is None
    stat = [(n_tiles, heads, 16, TILE), (n_tiles, heads, dim, TILE)]
    if last:
        out_shape = [jax.ShapeDtypeStruct(q[1].shape, jnp.bfloat16)] * 2
    else:
        out_shape = [jax.ShapeDtypeStruct(shape, jnp.float32) for shape in stat]
    state = () if first else tuple(state)
    any_spec = pl.BlockSpec(memory_space=pl.ANY)
    smem = pl.BlockSpec(memory_space=pltpu.SMEM)
    rows = 2 * (kvs[0].shape[0] // 4 // 128 * 128)
    items = 2 * n_tiles * 2 * n_src
    n_front = 3 + 2 + n_src
    aliases = {n_front + i: i for i in range(2)} if not first and not last else {}
    return pl.pallas_call(
        functools.partial(attend_kernel, masks, group, first, last),
        out_shape=out_shape,
        in_specs=[smem] * 3 + [any_spec] * (2 + n_src + len(state)),
        out_specs=[any_spec] * 2,
        scratch_shapes=[
            pltpu.VMEM((n_tiles,) + q[1].shape[1:], jnp.bfloat16),
            *[pltpu.VMEM((n_src, rows, dim), jnp.bfloat16)] * 2,
            pltpu.VMEM((heads, BLOCK, TILE), jnp.float32),
            pltpu.VMEM((heads, 8, TILE), jnp.float32),
            *[pltpu.VMEM(shape, jnp.float32) for shape in stat],
            pltpu.VMEM(((n_tiles,) + q[1].shape[1:]) if last else (8, 128), jnp.bfloat16),
            *[pltpu.SMEM((items,), jnp.int32)] * 4,
            pltpu.SMEM((n_tiles + 1,), jnp.int32),
            pltpu.SemaphoreType.DMA((2 + 2 * n_src,)),
            pltpu.SemaphoreType.DMA((2, n_tiles)),
            pltpu.SemaphoreType.DMA((2, n_tiles)),
        ],
        input_output_aliases=aliases,
        compiler_params=pltpu.CompilerParams(vmem_limit_bytes=60 * 1024 * 1024),
        cost_estimate=pl.CostEstimate(flops=n_src * 10**10, bytes_accessed=20 << 20, transcendentals=0),
    )(rank, cq, cnt, *q, *kvs, *state)


def solution(mesh):
    size_cx, size_cy = mesh.shape['cx'], mesh.shape['cy']
    group = size_cx * size_cy
    seq_spec = P(('dp', 'cx', 'cy'), None, None)

    def swap(array, mask):
        pairs = []
        for y in range(size_cy):
            for x in range(size_cx):
                other = (x * size_cy + y) ^ mask
                pairs.append((y * size_cx + x, (other % size_cy) * size_cx + other // size_cy))
        return lax.ppermute(array, ('cy', 'cx'), pairs)

    def per_device(q_loc, k_loc, v_loc, doc_loc):
        tok, heads, dim = q_loc.shape
        kv_heads = k_loc.shape[1]
        per_kv = heads // kv_heads
        piece, half_tiles = tok // 2, tok // TILE
        rank = lax.axis_index('cx') * size_cy + lax.axis_index('cy')
        core = (rank // 2) % 2

        def pick(array, index):
            return lax.dynamic_index_in_dim(array, index, 0, keepdims=False)

        cnt = jnp.sum(doc_loc.reshape(2, 1, piece) < jnp.arange(DOCS)[None, :, None], axis=-1).astype(jnp.int32).reshape(-1)
        digits = jnp.stack([cnt // 64, cnt % 64]).astype(jnp.bfloat16)
        digits = jnp.pad(digits, ((0, 14), (0, dim - digits.shape[1])))
        k_heads = k_loc.transpose(1, 0, 2)
        v_heads = v_loc.reshape(tok // 128, 128, kv_heads, dim).transpose(2, 0, 3, 1).reshape(kv_heads, tok, dim)
        kv = jnp.concatenate([k_heads, v_heads, jnp.broadcast_to(digits, (kv_heads,) + digits.shape)], axis=1)
        kv_mine, kv_other = pick(kv, core), pick(kv, 1 - core)

        def tile_heads(index):
            half = lax.dynamic_index_in_dim(q_loc.reshape(tok, kv_heads, per_kv, dim), index, 1, keepdims=False)
            return half.reshape(half_tiles, TILE, per_kv, dim).transpose(0, 2, 1, 3)

        q = (tile_heads(core), swap(tile_heads(1 - core), 2))
        kvs = {0: kv_mine}

        def fetch(masks, mine, other):
            for mask in masks:
                kvs[mask] = swap(other if mask & 2 else mine, mask)

        fetch((2, 4, 6, 1, 3), kv_mine, kv_other)

        def counts(masks):
            rows = jnp.stack([kvs[i][2 * tok:2 * tok + 2, :2 * DOCS] for i in masks]).astype(jnp.float32)
            return (rows[:, 0] * 64 + rows[:, 1]).astype(jnp.int32).reshape(-1)

        cq = counts((0, 2))

        def stage(masks, state, last):
            return attend(masks, group, rank[None], cq, counts(masks), q, [kvs[i] for i in masks], state, last)

        state = stage((0, 2), None, False)
        near, far = (4, 6, 1, 3), (5, 7)
        state, held, late = lax.optimization_barrier((state, [kvs[i] for i in near], (kv_mine, kv_other)))
        kvs.update(zip(near, held))
        fetch(far, *late)
        state = stage(near, state, False)
        state, held = lax.optimization_barrier((state, [kvs[i] for i in far]))
        kvs.update(zip(far, held))
        o_mine, o_other = stage(far, state, True)
        o_back = swap(o_other, 2)
        even = core == 0
        out = jnp.stack([jnp.where(even, o_mine, o_back), jnp.where(even, o_back, o_mine)])
        return out.transpose(1, 3, 0, 2, 4).reshape(tok, heads, dim)

    return jax.shard_map(per_device, mesh=mesh, in_specs=(seq_spec, seq_spec, seq_spec, P(('dp', 'cx', 'cy'))), out_specs=seq_spec, check_vma=False)
```

```python
import functools

import jax
import jax.numpy as jnp
from jax import lax
from jax.experimental import pallas as pl
from jax.experimental.pallas import tpu as pltpu
from jax.sharding import PartitionSpec as P

FLOOR = -1e30
MASKED = -3e38
LOG2E = 1.4426950408889634
DOCS = 6
TILE = 512
BLOCK = 512
CHUNK = 256


def fold8(x, op):
    return op(x.reshape(x.shape[0] // 8, 8, x.shape[1]), axis=0)


def attend_kernel(masks, group, first, last, rank_ref, cq_ref, cnt_ref, *rest):
    n_src = len(masks)
    q_hbm, rest = rest[:2], rest[2:]
    kv_hbm, rest = rest[:n_src], rest[n_src:]
    if not first:
        state_in, rest = rest[:2], rest[2:]
    outs, rest = rest[:2], rest[2:]
    q_ref, k_ref, v_ref, s_ref, cap_ref, mx_ref, ml_ref, acc_ref, o_ref, it_tile, it_sp, it_start, it_mask, it_from, sems, in_sems, out_sems = rest
    n_tiles, heads = q_ref.shape[0], q_ref.shape[1]
    piece = k_ref.shape[1] // 2
    tiles_per_piece = piece // TILE
    scale = q_ref.shape[-1] ** -0.5 * LOG2E
    rank = rank_ref[0]
    half_tiles = n_tiles // 2

    loads = [
        pltpu.make_async_copy(q_hbm[0], q_ref.at[pl.ds(0, half_tiles)], sems.at[0]),
        pltpu.make_async_copy(q_hbm[1], q_ref.at[pl.ds(half_tiles, half_tiles)], sems.at[1]),
    ]
    for src in range(n_src):
        loads.append(pltpu.make_async_copy(kv_hbm[src].at[pl.ds(0, 2 * piece)], k_ref.at[src], sems.at[2 + 2 * src]))
        loads.append(pltpu.make_async_copy(kv_hbm[src].at[pl.ds(2 * piece, 2 * piece)], v_ref.at[src], sems.at[3 + 2 * src]))
    for copy in loads:
        copy.start()

    def doc_of(tile, token):
        first_of = (tile // tiles_per_piece) * DOCS
        return sum((token >= cq_ref[first_of + d]).astype(jnp.int32) for d in range(1, DOCS))

    def list_tile(tile, count):
        it_from[tile] = count
        q_rank = jnp.where(tile < half_tiles, rank, rank ^ 2)
        q_piece = jnp.where((tile // tiles_per_piece) % 2 == 0, q_rank, 2 * group - 1 - q_rank)
        off = (tile % tiles_per_piece) * TILE
        d_first, d_last = doc_of(tile, off), doc_of(tile, off + TILE - 1)
        for sp in range(2 * n_src):
            src_rank = rank ^ masks[sp // 2]
            k_piece = src_rank if sp % 2 == 0 else 2 * group - 1 - src_rank
            lo, lo_last = cnt_ref[sp * DOCS + d_first], cnt_ref[sp * DOCS + d_last]
            diag = k_piece == q_piece
            hi = jnp.where(diag, off + TILE, piece)
            need = jnp.where(jnp.logical_and(k_piece <= q_piece, lo < hi), hi - (lo // 128) * 128, 0)
            blocks = (need + BLOCK - 1) // BLOCK
            start0 = jnp.maximum(hi - BLOCK * blocks, 0)

            def add(i, at, sp=sp, start0=start0, diag=diag, lo_last=lo_last):
                start = start0 + i * BLOCK
                it_tile[at] = tile
                it_sp[at] = sp
                it_start[at] = start
                cut = jnp.logical_or(start < lo_last, jnp.logical_and(diag, start + BLOCK > off + 1))
                it_mask[at] = jnp.where(cut, jnp.where(diag, 2, 1), 0)
                return at + 1

            count = lax.fori_loop(0, blocks, add, count)
        return count

    count = lax.fori_loop(0, n_tiles, list_tile, 0)
    it_from[n_tiles] = count

    def state_copies(tile, sem, inward):
        pairs = ((0, ml_ref), (1, acc_ref))
        if inward:
            return [pltpu.make_async_copy(state_in[i].at[tile], ref.at[tile], sem.at[i, tile]) for i, ref in pairs]
        return [pltpu.make_async_copy(ref.at[tile], outs[i].at[tile], sem.at[i, tile]) for i, ref in pairs]

    def used(tile):
        return it_from[tile + 1] > it_from[tile]

    def each_tile(fn):
        def one(tile, carry):
            if last:
                fn(tile)
            else:
                pl.when(used(tile))(lambda: fn(tile))
            return carry

        lax.fori_loop(0, n_tiles, one, 0)

    if first:
        ml_ref[:, :, 0:8, :] = jnp.zeros(ml_ref.shape[:2] + (8, TILE), jnp.float32)
        ml_ref[:, :, 8:16, :] = jnp.full(ml_ref.shape[:2] + (8, TILE), FLOOR, jnp.float32)
        acc_ref[...] = jnp.zeros_like(acc_ref)
    else:
        def fetch(tile):
            for copy in state_copies(tile, in_sems, True):
                copy.start()

        each_tile(fetch)
    for copy in loads:
        copy.wait()

    n_chunks = BLOCK // CHUNK

    def column(sp, start, j):
        return pl.ds(pl.multiple_of((sp % 2) * piece + start + j * CHUNK, 128), CHUNK)

    def values(sp, start, j):
        base = (sp % 2) * piece + start + j * CHUNK
        parts = [v_ref[sp // 2, pl.ds(pl.multiple_of(base + i * 128, 128), 128), :] for i in range(CHUNK // 128)]
        return jnp.concatenate(parts, axis=1)

    def set_caps(t):
        tile, sp, start = it_tile[t], it_sp[t], it_start[t]
        token = lax.broadcasted_iota(jnp.int32, (1, TILE), 1) + (tile % tiles_per_piece) * TILE
        low = jnp.full_like(token, cnt_ref[sp * DOCS])
        for d in range(1, DOCS):
            low = jnp.where(token >= cq_ref[(tile // tiles_per_piece) * DOCS + d], cnt_ref[sp * DOCS + d], low)
        low = low - start
        high = jnp.where(it_mask[t] == 2, token, piece) - start
        for j in range(n_chunks):
            row = lax.broadcasted_iota(jnp.int32, (CHUNK, TILE), 0) + j * CHUNK
            keep = jnp.logical_and(row >= low, row <= high)
            cap_ref[j * CHUNK:(j + 1) * CHUNK, :] = jnp.where(keep, jnp.inf, MASKED)

    def score(t, h, j, masked):
        s = lax.dot_general(
            k_ref[it_sp[t] // 2, column(it_sp[t], it_start[t], j), :], q_ref[it_tile[t], h],
            (((1,), (1,)), ((), ())), preferred_element_type=jnp.float32,
        )
        if masked:
            s = jnp.minimum(s, cap_ref[j * CHUNK:(j + 1) * CHUNK, :])
        s_ref[h, j * CHUNK:(j + 1) * CHUNK, :] = s
        return fold8(s, jnp.max)

    @pl.when(count > 0)
    def prologue():
        set_caps(0)
        for h in range(heads):
            mx_ref[h] = functools.reduce(jnp.maximum, [score(0, h, j, True) for j in range(n_chunks)])

    def body(t, nxt, masked):
        tile, sp, start = it_tile[t], it_sp[t], it_start[t]
        if masked:
            set_caps(nxt)
        for h in range(heads):
            m_old = ml_ref[tile, h, 8:9, :]
            m_new = jnp.maximum(m_old, jnp.max(mx_ref[h], axis=0, keepdims=True) * scale)
            rescale = jnp.exp2(m_old - m_new)
            ml_ref[tile, h, 8:9, :] = m_new
            total = ml_ref[tile, h, 0:8, :] * rescale
            prods, tops = [], []
            for j in range(n_chunks):
                p = jnp.exp2(s_ref[h, j * CHUNK:(j + 1) * CHUNK, :] * scale - m_new)
                total = total + fold8(p, jnp.sum)
                prods.append(jnp.dot(values(sp, start, j), p.astype(jnp.bfloat16), preferred_element_type=jnp.float32))
                tops.append(score(nxt, h, j, masked))
            mx_ref[h] = functools.reduce(jnp.maximum, tops)
            ml_ref[tile, h, 0:8, :] = total
            acc_ref[tile, h] = acc_ref[tile, h] * rescale + functools.reduce(jnp.add, prods)

    def step(t, carry):
        nxt = jnp.minimum(t + 1, count - 1)
        masked = it_mask[nxt] > 0
        pl.when(masked)(lambda: body(t, nxt, True))
        pl.when(jnp.logical_not(masked))(lambda: body(t, nxt, False))
        return carry

    def out_copy(tile, dst, base):
        return pltpu.make_async_copy(o_ref.at[tile], dst.at[tile - base], out_sems.at[0, tile])

    def send_out(tile, act):
        pl.when(tile < half_tiles)(lambda: act(out_copy(tile, outs[0], 0)))
        pl.when(tile >= half_tiles)(lambda: act(out_copy(tile, outs[1], half_tiles)))

    def run_tile(tile):
        if not first:
            for copy in state_copies(tile, in_sems, True):
                copy.wait()
        lax.fori_loop(it_from[tile], it_from[tile + 1], step, 0)
        if last:
            for h in range(heads):
                inverse = 1.0 / jnp.sum(ml_ref[tile, h, 0:8, :], axis=0, keepdims=True)
                o_ref[tile, h] = (acc_ref[tile, h] * inverse).T.astype(o_ref.dtype)
            send_out(tile, lambda copy: copy.start())
        else:
            for copy in state_copies(tile, out_sems, False):
                copy.start()

    each_tile(run_tile)

    def settle(tile):
        if last:
            send_out(tile, lambda copy: copy.wait())
        else:
            for copy in state_copies(tile, out_sems, False):
                copy.wait()

    each_tile(settle)


def attend(masks, group, rank, cq, cnt, q, kvs, state, last):
    half_tiles, heads, _, dim = q[1].shape
    n_tiles, n_src = 2 * half_tiles, len(masks)
    first = state is None
    stat = [(n_tiles, heads, 16, TILE), (n_tiles, heads, dim, TILE)]
    if last:
        out_shape = [jax.ShapeDtypeStruct(q[1].shape, jnp.bfloat16)] * 2
    else:
        out_shape = [jax.ShapeDtypeStruct(shape, jnp.float32) for shape in stat]
    state = () if first else tuple(state)
    any_spec = pl.BlockSpec(memory_space=pl.ANY)
    smem = pl.BlockSpec(memory_space=pltpu.SMEM)
    rows = 2 * (kvs[0].shape[0] // 4 // 128 * 128)
    items = 2 * n_tiles * 2 * n_src
    n_front = 3 + 2 + n_src
    aliases = {n_front + i: i for i in range(2)} if not first and not last else {}
    return pl.pallas_call(
        functools.partial(attend_kernel, masks, group, first, last),
        out_shape=out_shape,
        in_specs=[smem] * 3 + [any_spec] * (2 + n_src + len(state)),
        out_specs=[any_spec] * 2,
        scratch_shapes=[
            pltpu.VMEM((n_tiles,) + q[1].shape[1:], jnp.bfloat16),
            *[pltpu.VMEM((n_src, rows, dim), jnp.bfloat16)] * 2,
            pltpu.VMEM((heads, BLOCK, TILE), jnp.float32),
            pltpu.VMEM((BLOCK, TILE), jnp.float32),
            pltpu.VMEM((heads, 8, TILE), jnp.float32),
            *[pltpu.VMEM(shape, jnp.float32) for shape in stat],
            pltpu.VMEM(((n_tiles,) + q[1].shape[1:]) if last else (8, 128), jnp.bfloat16),
            *[pltpu.SMEM((items,), jnp.int32)] * 4,
            pltpu.SMEM((n_tiles + 1,), jnp.int32),
            pltpu.SemaphoreType.DMA((2 + 2 * n_src,)),
            pltpu.SemaphoreType.DMA((2, n_tiles)),
            pltpu.SemaphoreType.DMA((2, n_tiles)),
        ],
        input_output_aliases=aliases,
        compiler_params=pltpu.CompilerParams(vmem_limit_bytes=60 * 1024 * 1024),
        cost_estimate=pl.CostEstimate(flops=n_src * 10**10, bytes_accessed=20 << 20, transcendentals=0),
    )(rank, cq, cnt, *q, *kvs, *state)


def solution(mesh):
    size_cx, size_cy = mesh.shape['cx'], mesh.shape['cy']
    group = size_cx * size_cy
    seq_spec = P(('dp', 'cx', 'cy'), None, None)

    def swap(array, mask):
        pairs = []
        for y in range(size_cy):
            for x in range(size_cx):
                other = (x * size_cy + y) ^ mask
                pairs.append((y * size_cx + x, (other % size_cy) * size_cx + other // size_cy))
        return lax.ppermute(array, ('cy', 'cx'), pairs)

    def per_device(q_loc, k_loc, v_loc, doc_loc):
        tok, heads, dim = q_loc.shape
        kv_heads = k_loc.shape[1]
        per_kv = heads // kv_heads
        piece, half_tiles = tok // 2, tok // TILE
        rank = lax.axis_index('cx') * size_cy + lax.axis_index('cy')
        core = (rank // 2) % 2

        def pick(array, index):
            return lax.dynamic_index_in_dim(array, index, 0, keepdims=False)

        cnt = jnp.sum(doc_loc.reshape(2, 1, piece) < jnp.arange(DOCS)[None, :, None], axis=-1).astype(jnp.int32).reshape(-1)
        digits = jnp.stack([cnt // 64, cnt % 64]).astype(jnp.bfloat16)
        digits = jnp.pad(digits, ((0, 14), (0, dim - digits.shape[1])))
        k_heads = k_loc.transpose(1, 0, 2)
        v_heads = v_loc.reshape(tok // 128, 128, kv_heads, dim).transpose(2, 0, 3, 1).reshape(kv_heads, tok, dim)
        kv = jnp.concatenate([k_heads, v_heads, jnp.broadcast_to(digits, (kv_heads,) + digits.shape)], axis=1)
        kv_mine, kv_other = pick(kv, core), pick(kv, 1 - core)

        def tile_heads(index):
            half = lax.dynamic_index_in_dim(q_loc.reshape(tok, kv_heads, per_kv, dim), index, 1, keepdims=False)
            return half.reshape(half_tiles, TILE, per_kv, dim).transpose(0, 2, 1, 3)

        q = (tile_heads(core), swap(tile_heads(1 - core), 2))
        kvs = {0: kv_mine}

        def fetch(masks, mine, other):
            for mask in masks:
                kvs[mask] = swap(other if mask & 2 else mine, mask)

        fetch((2, 4, 6, 1, 3), kv_mine, kv_other)

        def counts(masks):
            rows = jnp.stack([kvs[i][2 * tok:2 * tok + 2, :2 * DOCS] for i in masks]).astype(jnp.float32)
            return (rows[:, 0] * 64 + rows[:, 1]).astype(jnp.int32).reshape(-1)

        cq = counts((0, 2))

        def stage(masks, state, last):
            return attend(masks, group, rank[None], cq, counts(masks), q, [kvs[i] for i in masks], state, last)

        state = stage((0, 2), None, False)
        near, far = (4, 6, 1, 3), (5, 7)
        state, held, late = lax.optimization_barrier((state, [kvs[i] for i in near], (kv_mine, kv_other)))
        kvs.update(zip(near, held))
        fetch(far, *late)
        state = stage(near, state, False)
        state, held = lax.optimization_barrier((state, [kvs[i] for i in far]))
        kvs.update(zip(far, held))
        o_mine, o_other = stage(far, state, True)
        o_back = swap(o_other, 2)
        even = core == 0
        out = jnp.stack([jnp.where(even, o_mine, o_back), jnp.where(even, o_back, o_mine)])
        return out.transpose(1, 3, 0, 2, 4).reshape(tok, heads, dim)

    return jax.shard_map(per_device, mesh=mesh, in_specs=(seq_spec, seq_spec, seq_spec, P(('dp', 'cx', 'cy'))), out_specs=seq_spec, check_vma=False)
```

```python
import functools

import jax
import jax.numpy as jnp
from jax import lax
from jax.experimental import pallas as pl
from jax.experimental.pallas import tpu as pltpu
from jax.sharding import PartitionSpec as P

FLOOR = -1e30
MASKED = -3e38
LOG2E = 1.4426950408889634
DOCS = 6
TILE = 512
BLOCK = 512
CHUNK = 256


def fold8(x, op):
    return op(x.reshape(x.shape[0] // 8, 8, x.shape[1]), axis=0)


def attend_kernel(masks, group, first, last, rank_ref, cq_ref, cnt_ref, *rest):
    n_src = len(masks)
    q_hbm, rest = rest[:2], rest[2:]
    kv_hbm, rest = rest[:n_src], rest[n_src:]
    if not first:
        state_in, rest = rest[:2], rest[2:]
    outs, rest = rest[:2], rest[2:]
    q_ref, k_ref, v_ref, s_ref, cap_ref, mx_ref, ml_ref, acc_ref, o_ref, it_tile, it_sp, it_start, it_mask, it_from, sems, in_sems, out_sems = rest
    n_tiles, heads = q_ref.shape[0], q_ref.shape[1]
    piece = k_ref.shape[1] // 2
    tiles_per_piece = piece // TILE
    scale = q_ref.shape[-1] ** -0.5 * LOG2E
    rank = rank_ref[0]
    half_tiles = n_tiles // 2

    loads = [
        pltpu.make_async_copy(q_hbm[0], q_ref.at[pl.ds(0, half_tiles)], sems.at[0]),
        pltpu.make_async_copy(q_hbm[1], q_ref.at[pl.ds(half_tiles, half_tiles)], sems.at[1]),
    ]
    for src in range(n_src):
        loads.append(pltpu.make_async_copy(kv_hbm[src].at[pl.ds(0, 2 * piece)], k_ref.at[src], sems.at[2 + 2 * src]))
        loads.append(pltpu.make_async_copy(kv_hbm[src].at[pl.ds(2 * piece, 2 * piece)], v_ref.at[src], sems.at[3 + 2 * src]))
    for copy in loads:
        copy.start()

    def doc_of(tile, token):
        first_of = (tile // tiles_per_piece) * DOCS
        return sum((token >= cq_ref[first_of + d]).astype(jnp.int32) for d in range(1, DOCS))

    def list_tile(tile, count):
        it_from[tile] = count
        q_rank = jnp.where(tile < half_tiles, rank, rank ^ 2)
        q_piece = jnp.where((tile // tiles_per_piece) % 2 == 0, q_rank, 2 * group - 1 - q_rank)
        off = (tile % tiles_per_piece) * TILE
        d_first, d_last = doc_of(tile, off), doc_of(tile, off + TILE - 1)
        for sp in range(2 * n_src):
            src_rank = rank ^ masks[sp // 2]
            k_piece = src_rank if sp % 2 == 0 else 2 * group - 1 - src_rank
            lo, lo_last = cnt_ref[sp * DOCS + d_first], cnt_ref[sp * DOCS + d_last]
            diag = k_piece == q_piece
            hi = jnp.where(diag, off + TILE, piece)
            need = jnp.where(jnp.logical_and(k_piece <= q_piece, lo < hi), hi - lo, 0)
            blocks = (need + BLOCK - 1) // BLOCK
            start0 = jnp.maximum(hi - BLOCK * blocks, 0)

            def add(i, at, sp=sp, start0=start0, diag=diag, lo_last=lo_last):
                start = start0 + i * BLOCK
                it_tile[at] = tile
                it_sp[at] = sp
                it_start[at] = start
                cut = jnp.logical_or(start < lo_last, jnp.logical_and(diag, start + BLOCK > off + 1))
                it_mask[at] = jnp.where(cut, jnp.where(diag, 2, 1), 0)
                return at + 1

            count = lax.fori_loop(0, blocks, add, count)
        return count

    count = lax.fori_loop(0, n_tiles, list_tile, 0)
    it_from[n_tiles] = count

    def state_copies(tile, sem, inward):
        pairs = ((0, ml_ref), (1, acc_ref))
        if inward:
            return [pltpu.make_async_copy(state_in[i].at[tile], ref.at[tile], sem.at[i, tile]) for i, ref in pairs]
        return [pltpu.make_async_copy(ref.at[tile], outs[i].at[tile], sem.at[i, tile]) for i, ref in pairs]

    def used(tile):
        return it_from[tile + 1] > it_from[tile]

    def each_tile(fn):
        def one(tile, carry):
            if last:
                fn(tile)
            else:
                pl.when(used(tile))(lambda: fn(tile))
            return carry

        lax.fori_loop(0, n_tiles, one, 0)

    if first:
        ml_ref[:, :, 0:8, :] = jnp.zeros(ml_ref.shape[:2] + (8, TILE), jnp.float32)
        ml_ref[:, :, 8:16, :] = jnp.full(ml_ref.shape[:2] + (8, TILE), FLOOR, jnp.float32)
        acc_ref[...] = jnp.zeros_like(acc_ref)
    else:
        def fetch(tile):
            for copy in state_copies(tile, in_sems, True):
                copy.start()

        each_tile(fetch)
    for copy in loads:
        copy.wait()

    n_chunks = BLOCK // CHUNK

    def column(sp, start, j):
        return pl.ds(pl.multiple_of((sp % 2) * piece + start + j * CHUNK, 128), CHUNK)

    def values(sp, start, j):
        base = (sp % 2) * piece + start + j * CHUNK
        parts = [v_ref[sp // 2, pl.ds(pl.multiple_of(base + i * 128, 128), 128), :] for i in range(CHUNK // 128)]
        return jnp.concatenate(parts, axis=1)

    def set_caps(t):
        tile, sp, start = it_tile[t], it_sp[t], it_start[t]
        token = lax.broadcasted_iota(jnp.int32, (1, TILE), 1) + (tile % tiles_per_piece) * TILE
        low = jnp.full_like(token, cnt_ref[sp * DOCS])
        for d in range(1, DOCS):
            low = jnp.where(token >= cq_ref[(tile // tiles_per_piece) * DOCS + d], cnt_ref[sp * DOCS + d], low)
        low = low - start
        high = jnp.where(it_mask[t] == 2, token, piece) - start
        for j in range(n_chunks):
            row = lax.broadcasted_iota(jnp.int32, (CHUNK, TILE), 0) + j * CHUNK
            keep = jnp.logical_and(row >= low, row <= high)
            cap_ref[j * CHUNK:(j + 1) * CHUNK, :] = jnp.where(keep, jnp.inf, MASKED)

    def score(t, h, j, masked):
        s = lax.dot_general(
            k_ref[it_sp[t] // 2, column(it_sp[t], it_start[t], j), :], q_ref[it_tile[t], h],
            (((1,), (1,)), ((), ())), preferred_element_type=jnp.float32,
        )
        if masked:
            s = jnp.minimum(s, cap_ref[j * CHUNK:(j + 1) * CHUNK, :])
        s_ref[h, j * CHUNK:(j + 1) * CHUNK, :] = s
        return fold8(s, jnp.max)

    @pl.when(count > 0)
    def prologue():
        set_caps(0)
        for h in range(heads):
            mx_ref[h] = functools.reduce(jnp.maximum, [score(0, h, j, True) for j in range(n_chunks)])

    def body(t, nxt, masked):
        tile, sp, start = it_tile[t], it_sp[t], it_start[t]
        if masked:
            set_caps(nxt)
        for h in range(heads):
            m_old = ml_ref[tile, h, 8:9, :]
            m_new = jnp.maximum(m_old, jnp.max(mx_ref[h], axis=0, keepdims=True) * scale)
            rescale = jnp.exp2(m_old - m_new)
            ml_ref[tile, h, 8:9, :] = m_new
            total = ml_ref[tile, h, 0:8, :] * rescale
            prods, tops = [], []
            for j in range(n_chunks):
                p = jnp.exp2(s_ref[h, j * CHUNK:(j + 1) * CHUNK, :] * scale - m_new)
                total = total + fold8(p, jnp.sum)
                prods.append(jnp.dot(values(sp, start, j), p.astype(jnp.bfloat16), preferred_element_type=jnp.float32))
                tops.append(score(nxt, h, j, masked))
            mx_ref[h] = functools.reduce(jnp.maximum, tops)
            ml_ref[tile, h, 0:8, :] = total
            acc_ref[tile, h] = acc_ref[tile, h] * rescale + functools.reduce(jnp.add, prods)

    def step(t, carry):
        nxt = jnp.minimum(t + 1, count - 1)
        masked = it_mask[nxt] > 0
        pl.when(masked)(lambda: body(t, nxt, True))
        pl.when(jnp.logical_not(masked))(lambda: body(t, nxt, False))
        return carry

    def out_copy(tile, dst, base):
        return pltpu.make_async_copy(o_ref.at[tile], dst.at[tile - base], out_sems.at[0, tile])

    def send_out(tile, act):
        pl.when(tile < half_tiles)(lambda: act(out_copy(tile, outs[0], 0)))
        pl.when(tile >= half_tiles)(lambda: act(out_copy(tile, outs[1], half_tiles)))

    def run_tile(tile):
        if not first:
            for copy in state_copies(tile, in_sems, True):
                copy.wait()
        lax.fori_loop(it_from[tile], it_from[tile + 1], step, 0)
        if last:
            for h in range(heads):
                inverse = 1.0 / jnp.sum(ml_ref[tile, h, 0:8, :], axis=0, keepdims=True)
                o_ref[tile, h] = (acc_ref[tile, h] * inverse).T.astype(o_ref.dtype)
            send_out(tile, lambda copy: copy.start())
        else:
            for copy in state_copies(tile, out_sems, False):
                copy.start()

    each_tile(run_tile)

    def settle(tile):
        if last:
            send_out(tile, lambda copy: copy.wait())
        else:
            for copy in state_copies(tile, out_sems, False):
                copy.wait()

    each_tile(settle)


def attend(masks, group, rank, cq, cnt, q, kvs, state, last):
    half_tiles, heads, _, dim = q[1].shape
    n_tiles, n_src = 2 * half_tiles, len(masks)
    first = state is None
    stat = [(n_tiles, heads, 16, TILE), (n_tiles, heads, dim, TILE)]
    if last:
        out_shape = [jax.ShapeDtypeStruct(q[1].shape, jnp.bfloat16)] * 2
    else:
        out_shape = [jax.ShapeDtypeStruct(shape, jnp.float32) for shape in stat]
    state = () if first else tuple(state)
    any_spec = pl.BlockSpec(memory_space=pl.ANY)
    smem = pl.BlockSpec(memory_space=pltpu.SMEM)
    rows = 2 * (kvs[0].shape[0] // 4 // 128 * 128)
    items = 2 * n_tiles * 2 * n_src
    n_front = 3 + 2 + n_src
    aliases = {n_front + i: i for i in range(2)} if not first and not last else {}
    return pl.pallas_call(
        functools.partial(attend_kernel, masks, group, first, last),
        out_shape=out_shape,
        in_specs=[smem] * 3 + [any_spec] * (2 + n_src + len(state)),
        out_specs=[any_spec] * 2,
        scratch_shapes=[
            pltpu.VMEM((n_tiles,) + q[1].shape[1:], jnp.bfloat16),
            *[pltpu.VMEM((n_src, rows, dim), jnp.bfloat16)] * 2,
            pltpu.VMEM((heads, BLOCK, TILE), jnp.float32),
            pltpu.VMEM((BLOCK, TILE), jnp.float32),
            pltpu.VMEM((heads, 8, TILE), jnp.float32),
            *[pltpu.VMEM(shape, jnp.float32) for shape in stat],
            pltpu.VMEM(((n_tiles,) + q[1].shape[1:]) if last else (8, 128), jnp.bfloat16),
            *[pltpu.SMEM((items,), jnp.int32)] * 4,
            pltpu.SMEM((n_tiles + 1,), jnp.int32),
            pltpu.SemaphoreType.DMA((2 + 2 * n_src,)),
            pltpu.SemaphoreType.DMA((2, n_tiles)),
            pltpu.SemaphoreType.DMA((2, n_tiles)),
        ],
        input_output_aliases=aliases,
        compiler_params=pltpu.CompilerParams(vmem_limit_bytes=60 * 1024 * 1024),
        cost_estimate=pl.CostEstimate(flops=n_src * 10**10, bytes_accessed=20 << 20, transcendentals=0),
    )(rank, cq, cnt, *q, *kvs, *state)


def solution(mesh):
    size_cx, size_cy = mesh.shape['cx'], mesh.shape['cy']
    group = size_cx * size_cy
    seq_spec = P(('dp', 'cx', 'cy'), None, None)

    def swap(array, mask):
        pairs = []
        for y in range(size_cy):
            for x in range(size_cx):
                other = (x * size_cy + y) ^ mask
                pairs.append((y * size_cx + x, (other % size_cy) * size_cx + other // size_cy))
        return lax.ppermute(array, ('cy', 'cx'), pairs)

    def per_device(q_loc, k_loc, v_loc, doc_loc):
        tok, heads, dim = q_loc.shape
        kv_heads = k_loc.shape[1]
        per_kv = heads // kv_heads
        piece, half_tiles = tok // 2, tok // TILE
        rank = lax.axis_index('cx') * size_cy + lax.axis_index('cy')
        core = (rank // 2) % 2

        def pick(array, index):
            return lax.dynamic_index_in_dim(array, index, 0, keepdims=False)

        cnt = jnp.sum(doc_loc.reshape(2, 1, piece) < jnp.arange(DOCS)[None, :, None], axis=-1).astype(jnp.int32).reshape(-1)
        digits = jnp.stack([cnt // 64, cnt % 64]).astype(jnp.bfloat16)
        digits = jnp.pad(digits, ((0, 14), (0, dim - digits.shape[1])))
        k_heads = k_loc.transpose(1, 0, 2)
        v_heads = v_loc.reshape(tok // 128, 128, kv_heads, dim).transpose(2, 0, 3, 1).reshape(kv_heads, tok, dim)
        kv = jnp.concatenate([k_heads, v_heads, jnp.broadcast_to(digits, (kv_heads,) + digits.shape)], axis=1)
        kv_mine, kv_other = pick(kv, core), pick(kv, 1 - core)

        def tile_heads(index):
            half = lax.dynamic_index_in_dim(q_loc.reshape(tok, kv_heads, per_kv, dim), index, 1, keepdims=False)
            return half.reshape(half_tiles, TILE, per_kv, dim).transpose(0, 2, 1, 3)

        q = (tile_heads(core), swap(tile_heads(1 - core), 2))
        kvs = {0: kv_mine}

        def fetch(masks, mine, other):
            for mask in masks:
                kvs[mask] = swap(other if mask & 2 else mine, mask)

        fetch((2, 4, 6, 1, 3), kv_mine, kv_other)

        def counts(masks):
            rows = jnp.stack([kvs[i][2 * tok:2 * tok + 2, :2 * DOCS] for i in masks]).astype(jnp.float32)
            return (rows[:, 0] * 64 + rows[:, 1]).astype(jnp.int32).reshape(-1)

        cq = counts((0, 2))

        def stage(masks, state, last):
            return attend(masks, group, rank[None], cq, counts(masks), q, [kvs[i] for i in masks], state, last)

        state = stage((0, 2), None, False)
        near, far = (4, 6, 1, 3), (5, 7)
        state, held, late = lax.optimization_barrier((state, [kvs[i] for i in near], (kv_mine, kv_other)))
        kvs.update(zip(near, held))
        fetch(far, *late)
        state = stage(near, state, False)
        state, held = lax.optimization_barrier((state, [kvs[i] for i in far]))
        kvs.update(zip(far, held))
        o_mine, o_other = stage(far, state, True)
        o_back = swap(o_other, 2)
        even = core == 0
        out = jnp.stack([jnp.where(even, o_mine, o_back), jnp.where(even, o_back, o_mine)])
        return out.transpose(1, 3, 0, 2, 4).reshape(tok, heads, dim)

    return jax.shard_map(per_device, mesh=mesh, in_specs=(seq_spec, seq_spec, seq_spec, P(('dp', 'cx', 'cy'))), out_specs=seq_spec, check_vma=False)
```
